32 devices in a mesh: row: 4 (over x, core), col: 8 (over z, y).
Axes of the slice: x: 2, y: 2, z: 4, core: 2. Of those that a mesh axis runs over, the one named last changes fastest.
Arguments:
- normed: bfloat16 [12288, 6144], P(('row', 'col')), may hold values from -6 to 6
- out_grad: bfloat16 [12288, 6144], P(('row', 'col')), may hold values from -0.125 to 0.125
- w_in: bfloat16 [6144, 48], replicated, may hold values from -0.078125 to 0.078125
- hidden_grad: bfloat16 [12288, 48], P(('row', 'col')), may hold values from -0.125 to 0.125
- qkv_grad: bfloat16 [12288, 64], P(('row', 'col')), may hold values from -0.125 to 0.125
- bucket_order: int32 [160], replicated, may hold values from 0 to 159, each once
Outputs:
- buckets: bfloat16 [160, 6144], replicated
The draws below stay inside these ranges and needn't reach their ends.
Inputs may be any that keep to these rules, and one draw needn't show every extreme that they name: bucket_order is a permutation of 0 to 159.
All inputs are finite; a program needn't handle non-finite values.
Results may differ from the reference program's by a relative error of at most 0.0044.
Values may be sent and summed in bfloat16 or wider, within the bound.
No kernel may reach another device: no remote copies, remote signals or barrier semaphores. Data moves between devices by JAX's collectives and lax.ppermute only.
A program may use at most 64 MiB of HBM per device.

```python
import jax
import jax.numpy as jnp
from jax import lax

D = 6144
QW = 64
HW = 48
TOK_DEV = 384
TOKENS = 12288
N_ROW = 4
N_COL = 8


def steps_of(own_key, shape, pieces, low, high):
    gain, own = 1.0, jax.random.fold_in(own_key, 6)
    for dim, shards_of in pieces:
        heights = jnp.exp(jax.random.uniform(jax.random.fold_in(own, dim), (shards_of,), jnp.float32, low / len(pieces), high / len(pieces)))
        gain = gain * jnp.repeat(heights, shape[dim] // shards_of).reshape([-1 if axis == dim else 1 for axis in range(len(shape))])
    return gain


def bell_draw(own_key, extent, scale, limit, cuts=(), held_as=jnp.bfloat16):
    values = jax.random.normal(own_key, extent, jnp.float32) * scale
    if len(cuts) > 0:
        values = steps_of(own_key, extent, cuts, -0.22, 0.18) * values
    return jnp.clip(values, min=-limit, max=limit).astype(held_as)


def setup_inputs(seed: int = 0) -> dict:
    seeds = jax.random.split(jax.random.key(seed), 7)
    normed = bell_draw(seeds[0], (TOKENS, D), 1.0, 6.0, ((0, 32),))
    out_grad = bell_draw(seeds[1], (TOKENS, D), ((TOK_DEV * N_ROW * N_COL) ** -0.5), 0.125, ((0, 32),))
    w_in = bell_draw(seeds[2], (D, HW), D ** -0.5, 0.078125)
    hidden_grad = bell_draw(seeds[3], (TOKENS, HW), ((TOK_DEV * N_ROW * N_COL) ** -0.5), 0.125, ((0, 32),))
    qkv_grad = bell_draw(seeds[4], (TOKENS, QW), ((TOK_DEV * N_ROW * N_COL) ** -0.5), 0.125, ((0, 32),))
    bucket_order = jax.random.permutation(seeds[5], QW + 2 * HW).astype(jnp.int32)
    return {"normed": normed, "out_grad": out_grad, "w_in": w_in, "hidden_grad": hidden_grad, "qkv_grad": qkv_grad, "bucket_order": bucket_order}


def reference(normed, out_grad, w_in, hidden_grad, qkv_grad, bucket_order):
    pre = jnp.dot(normed, w_in, preferred_element_type=jnp.float32)
    cdf = 0.5 * (1.0 + lax.erf(pre * 0.7071067811865476))
    pdf = jnp.exp(-0.5 * pre * pre) * 0.3989422804014327
    hidden = (pre * cdf).astype(jnp.bfloat16)
    pre_grad = (hidden_grad.astype(jnp.float32) * (cdf + pre * pdf)).astype(jnp.bfloat16)
    grad_qkv = jnp.dot(qkv_grad.T, normed, preferred_element_type=jnp.float32)
    grad_in = jnp.dot(pre_grad.T, normed, preferred_element_type=jnp.float32)
    grad_out = jnp.dot(hidden.T, out_grad, preferred_element_type=jnp.float32)
    stacked = jnp.concatenate([grad_qkv, grad_in, grad_out], axis=0)
    return jnp.take(stacked, bucket_order.astype(jnp.int32), axis=0).astype(jnp.bfloat16)
```

```python
import functools

import jax
import jax.numpy as jnp
from jax import lax
from jax.experimental import pallas as pl
from jax.experimental.pallas import tpu as pltpu
from jax.sharding import Mesh
from jax.sharding import PartitionSpec as P

F32, BF16 = jnp.float32, jnp.bfloat16
NEAR = ("x", "c1", "c0")
GROUP = 8
ANY = pl.BlockSpec(memory_space=pl.ANY)
SMEM = pl.BlockSpec(memory_space=pltpu.SMEM)
VMEM = pl.BlockSpec(memory_space=pltpu.VMEM)


def near_core(value):
    return pltpu.with_memory_space_constraint(value, pltpu.VMEM)


def in_hbm(value):
    return pltpu.with_memory_space_constraint(value, pltpu.HBM)


def nt(a, b):
    return lax.dot_general(a, b, (((1,), (1,)), ((), ())), preferred_element_type=F32)


def nn(a, b):
    return lax.dot_general(a, b, (((1,), (0,)), ((), ())), preferred_element_type=F32)


def grads_kernel(half_ref, w_hbm, hg_hbm, qg_hbm, x_hbm, og_hbm, keep_ref, send_ref, w_ref, hg_ref, qg_ref, x_ref, og_ref, stk, sems, small):
    pieces, half, width = keep_ref.shape
    per = 2
    chunk = per * width
    n = pieces // per
    qw, hw = qg_ref.shape[0], hg_ref.shape[0]
    early = []
    for i, (src, dst) in enumerate(((w_hbm, w_ref), (qg_hbm, qg_ref), (hg_hbm, hg_ref))):
        early.append(pltpu.make_async_copy(src, dst, small.at[i]))
        early[-1].start()
    copies = []
    for i, (src, dst) in enumerate(((x_hbm, x_ref), (og_hbm, og_ref))):
        for c in range(n):
            cols = pl.ds(c * chunk, chunk)
            copies.append(pltpu.make_async_copy(src.at[:, cols], dst.at[:, cols], sems.at[i * n + c]))
            copies[-1].start()

    def put(row, c, value):
        done = 0
        while done < value.shape[0]:
            h, r = divmod(row + done, half)
            size = min(half - r, value.shape[0] - done)
            for p in range(per):
                stk[h, c * per + p, r : r + size, :] = value[done : done + size, p * width : (p + 1) * width]
            done += size

    for copy in early:
        copy.wait()
    pre = jnp.zeros(hg_ref.shape, F32)
    for c in range(n):
        copies[c].wait()
        cols = slice(c * chunk, (c + 1) * chunk)
        pre = pre + nt(w_ref[:, cols], x_ref[:, cols])
        put(0, c, nn(qg_ref[...], x_ref[:, cols]))
    cdf = 0.5 * (1.0 + lax.erf(pre * 0.7071067811865476))
    pdf = jnp.exp(-0.5 * pre * pre) * 0.3989422804014327
    hidden = (pre * cdf).astype(BF16)
    pre_grad = (hg_ref[...].astype(F32) * (cdf + pre * pdf)).astype(BF16)
    for c in range(n):
        cols = slice(c * chunk, (c + 1) * chunk)
        put(qw, c, nn(pre_grad, x_ref[:, cols]))
    for c in range(n):
        copies[n + c].wait()
        cols = slice(c * chunk, (c + 1) * chunk)
        put(qw + hw, c, nn(hidden, og_ref[:, cols]))
    mine = half_ref[0]
    for p in range(pieces):
        keep_ref[p] = stk[mine, p]
        send_ref[p] = stk[1 - mine, p].astype(BF16)


def split_kernel(near_ref, keep_ref, got_ref, own_ref, *send_refs):
    per = own_ref.shape[0]
    me = near_ref[0]
    for mask in range(GROUP):
        base = (me ^ mask) * per
        for p in range(per):
            value = keep_ref[base + p] + got_ref[base + p].astype(F32)
            if mask == 0:
                own_ref[p] = value
            else:
                send_refs[mask - 1][p] = value.astype(BF16)


def sum_kernel(own_ref, *refs):
    *got, out_ref = refs
    for p in range(own_ref.shape[0]):
        value = own_ref[p]
        for g in got:
            value = value + g[p].astype(F32)
        out_ref[p] = value.astype(BF16)


def order_kernel(where_ref, order_ref, *refs):
    pieces, out_hbm, buf, sems = refs[:-3], refs[-3], refs[-2], refs[-1]
    per, half, width = pieces[0].shape
    rows = 2 * half
    mine, me = where_ref[0], where_ref[1]
    order = order_ref[...]
    ids = lax.broadcasted_iota(jnp.int32, (half, rows), 0)
    near = (ids + mine * half == order).astype(F32).T.astype(BF16)
    far = (ids + (1 - mine) * half == order).astype(F32).T.astype(BF16)
    copies = []
    for mask in range(GROUP):
        for p in range(per):
            slot = mask * per + p
            value = nn(near, pieces[mask][p]) + nn(far, pieces[GROUP + mask][p])
            buf[slot] = value.astype(BF16)
            col = pl.multiple_of(((me ^ mask) * per + p) * width, 128)
            copies.append(pltpu.make_async_copy(buf.at[slot], out_hbm.at[:, pl.ds(col, width)], sems.at[slot]))
            copies[-1].start()
    for copy in copies:
        copy.wait()


def local(outer, normed, out_grad, w_in, hidden_grad, qkv_grad, bucket_order):
    tok, d = normed.shape
    rows = bucket_order.shape[0]
    per = 2
    pieces, half = GROUP * per, rows // 2
    width = d // pieces
    mine = lax.axis_index("k").astype(jnp.int32)
    me = lax.axis_index(NEAR).astype(jnp.int32)
    piece = (per, half, width)
    full = (pieces, half, width)

    keep, send = pl.pallas_call(
        grads_kernel,
        out_shape=(pltpu.VMEM(full, F32), pltpu.VMEM(full, BF16)),
        in_specs=[SMEM] + [ANY] * 5,
        out_specs=(VMEM, VMEM),
        scratch_shapes=[
            pltpu.VMEM(w_in.shape[::-1], BF16),
            pltpu.VMEM(hidden_grad.shape[::-1], BF16),
            pltpu.VMEM(qkv_grad.shape[::-1], BF16),
            pltpu.VMEM((tok, d), BF16),
            pltpu.VMEM((tok, d), BF16),
            pltpu.VMEM((2,) + full, F32),
            pltpu.SemaphoreType.DMA((pieces,)),
            pltpu.SemaphoreType.DMA((3,)),
        ],
        compiler_params=pltpu.CompilerParams(vmem_limit_bytes=28 << 20),
        name="grads",
    )(mine[None], *map(in_hbm, (w_in.T, hidden_grad.T, qkv_grad.T, normed, out_grad)))

    swap = [(0, 1), (1, 0)]
    got = lax.ppermute(send, "k", swap)
    own, *sends = pl.pallas_call(
        split_kernel,
        out_shape=(pltpu.VMEM(piece, F32),) + (pltpu.VMEM(piece, BF16),) * (GROUP - 1),
        in_specs=[SMEM, VMEM, VMEM],
        out_specs=(VMEM,) * GROUP,
        compiler_params=pltpu.CompilerParams(vmem_limit_bytes=12 << 20),
        name="split",
    )(me[None], near_core(keep), near_core(got))

    def flip(value, mask):
        return lax.ppermute(value, NEAR, [(i, i ^ mask) for i in range(GROUP)])

    parts = [flip(s, mask + 1) for mask, s in enumerate(sends)]
    part = pl.pallas_call(
        sum_kernel,
        out_shape=pltpu.VMEM(piece, BF16),
        in_specs=[VMEM] * GROUP,
        out_specs=VMEM,
        compiler_params=pltpu.CompilerParams(vmem_limit_bytes=12 << 20),
        name="sum",
    )(*map(near_core, (own, *parts)))
    total = part.astype(F32) + lax.ppermute(part, "c2", swap).astype(F32)
    if outer:
        total = lax.psum(total, ("rh", "ch"))
    total = total.astype(BF16)

    near = [total] + [flip(total, mask) for mask in range(1, GROUP)]
    far = [lax.ppermute(v, "k", swap) for v in near]
    return pl.pallas_call(
        order_kernel,
        out_shape=jax.ShapeDtypeStruct((rows, d), BF16),
        in_specs=[SMEM, VMEM] + [VMEM] * (2 * GROUP),
        out_specs=ANY,
        scratch_shapes=[pltpu.VMEM((pieces, rows, width), BF16), pltpu.SemaphoreType.DMA((pieces,))],
        compiler_params=pltpu.CompilerParams(vmem_limit_bytes=16 << 20),
        name="order",
    )(jnp.stack([mine, me]), bucket_order.reshape(1, rows), *map(near_core, near + far))


def solution(mesh):
    n_row, n_col = mesh.devices.shape
    axes = ("rh", "x", "k", "ch", "c2", "c1", "c0")
    fine = Mesh(mesh.devices.reshape(n_row // 4, 2, 2, n_col // 8, 2, 2, 2), axes)
    tokens = P(axes, None)
    return jax.shard_map(
        functools.partial(local, n_row * n_col > 32),
        mesh=fine,
        in_specs=(tokens, tokens, P(), tokens, tokens, P()),
        out_specs=P(),
        check_vma=False,
    )
```
